32 devices in a mesh: head: 8 (over y, x, core), seq: 4 (over z).
Axes of the slice: x: 2, y: 2, z: 4, core: 2. Of those that a mesh axis runs over, the one named last changes fastest.
Arguments:
- query_rows: bfloat16 [512, 16384], P('seq', 'head'), may hold values from -512 to 512
- key_rows: bfloat16 [512, 1024], P('seq'), may hold values from -32 to 32
- value_rows: bfloat16 [512, 1024], P('seq'), may hold values from -6 to 6
- positions: int32 [512], P('seq'), may hold values from 0 to 511, as said below
Outputs:
- attended: bfloat16 [512, 16384], P('seq', 'head')
- hessian: float32 [16384, 16384], P('head', 'seq')
The draws below stay inside these ranges and needn't reach their ends.
Inputs may be any that keep to these rules, and one draw needn't show every extreme that they name: Each aligned block of 4 spans of 128 tokens is one sequence; each span holds 128 consecutive ascending positions starting at a multiple of 128, and the sequence's spans together hold every position 0 to 511 once.
All inputs are finite; a program needn't handle non-finite values.
Results may differ from the reference program's by a relative error of at most 0.0037.
Values may be sent and summed in bfloat16 or wider, within the bound.
A program may use at most 128 MiB of HBM per device.

```python
import jax
import jax.numpy as jnp
from jax import lax

HEADS = 128
KVH = 8
HD = 128
TOK_DEV = 128
SPANS = 4
LENGTH = 512
TOKENS = 512


def draw_key_rows(key, part):
    noise_key = jax.random.fold_in(key, 1)
    drawn = jnp.clip(jax.random.normal(noise_key, (TOKENS, KVH * HD), jnp.float32), -4.0, 4.0)
    return drawn.astype(jnp.bfloat16)


def draw_query_rows(key, part):
    noise_key = jax.random.fold_in(key, 2)
    drawn = jnp.clip(jax.random.normal(noise_key, (TOKENS, HEADS * HD), jnp.float32), -4.0, 4.0)
    return drawn.astype(jnp.bfloat16)


def draw_positions(key, part):
    sequence_keys = jax.random.split(jax.random.fold_in(key, 5), TOKENS // LENGTH)
    slots = jax.vmap(lambda single: jax.random.permutation(single, SPANS))(sequence_keys)
    within = jnp.arange(TOK_DEV, dtype=jnp.int32)
    return (slots[:, :, None].astype(jnp.int32) * TOK_DEV + within[None, None, :]).reshape(TOKENS)


def shard_levels(own_key, shape, shards, least, largest):
    level = 1.0
    for position, shards_of in shards:
        steps = jax.random.uniform(jax.random.fold_in(jax.random.fold_in(own_key, 6), position), (shards_of,), jnp.float32, least / len(shards), largest / len(shards))
        level = level * jnp.repeat(jnp.exp(steps), shape[position] // shards_of).reshape((-1,) + (1,) * (len(shape) - 1 - position))
    return level


def noise(rng, dims, spread, limit, cuts=(), kind=jnp.bfloat16):
    entries = jax.random.normal(rng, dims, jnp.float32) * spread
    if len(cuts) > 0:
        entries = shard_levels(rng, dims, cuts, -0.22, 0.18) * entries
    return jnp.clip(entries, min=-limit, max=limit).astype(kind)


def setup_inputs(seed: int = 0) -> dict:
    splits = jax.random.split(jax.random.key(seed), 5)
    query_rows = draw_query_rows(jax.random.fold_in(splits[4], 71), 0)
    key_rows = draw_key_rows(jax.random.fold_in(splits[4], 71), 0)
    value_rows = noise(splits[2], (TOKENS, KVH * HD), 1.0, 6.0, ((0, 4),))
    positions = draw_positions(jax.random.fold_in(splits[4], 71), 0)
    return {"query_rows": query_rows, "key_rows": key_rows, "value_rows": value_rows, "positions": positions}


def reference(query_rows, key_rows, value_rows, positions):
    group_size = HEADS // KVH
    sequence_count = TOKENS // LENGTH
    score_scale = HD ** -0.5
    queries = query_rows.reshape(sequence_count, LENGTH, KVH, group_size, HD)
    queries = jnp.transpose(queries, (0, 2, 3, 1, 4)).reshape(sequence_count, KVH, group_size * LENGTH, HD)
    key_heads = jnp.transpose(key_rows.reshape(sequence_count, LENGTH, KVH, HD), (0, 2, 1, 3))
    value_heads = jnp.transpose(value_rows.reshape(sequence_count, LENGTH, KVH, HD), (0, 2, 1, 3))
    places = positions.reshape(sequence_count, LENGTH)

    def head_group(inputs):
        query_block, key_block, value_block, visible = inputs
        scores = jnp.dot(query_block, key_block.T, preferred_element_type=jnp.float32) * score_scale
        scores = scores.reshape(group_size, LENGTH, LENGTH)
        masked = jnp.where(visible[None], scores, -jnp.inf)
        row_top = jnp.max(masked, axis=2, keepdims=True)
        weights = jnp.exp(masked - row_top)
        weight_sum = jnp.sum(weights, axis=2, keepdims=True)
        mixed = jnp.dot(weights.astype(jnp.bfloat16).reshape(group_size * LENGTH, LENGTH), value_block,
                        preferred_element_type=jnp.float32)
        return (mixed.reshape(group_size, LENGTH, HD) / weight_sum).astype(jnp.bfloat16)

    def sequence_part(inputs):
        query_seq, key_seq, value_seq, place_seq = inputs
        visible = place_seq[None, :] <= place_seq[:, None]
        visible_all = jnp.broadcast_to(visible, (KVH, LENGTH, LENGTH))
        return lax.map(head_group, (query_seq, key_seq, value_seq, visible_all))

    outputs = lax.map(sequence_part, (queries, key_heads, value_heads, places))
    attended = jnp.transpose(outputs, (0, 3, 1, 2, 4)).reshape(TOKENS, HEADS * HD)
    hessian = jnp.dot(attended.T, attended, preferred_element_type=jnp.float32)
    return attended, hessian
```

```python
import functools

import jax
import jax.numpy as jnp
from jax import lax
from jax.experimental import pallas as pl
from jax.experimental.pallas import tpu as pltpu
from jax.sharding import PartitionSpec as P

HEADS = 128
KVH = 8
HD = 128
SPANS = 4
MESH = pl.DeviceIdType.MESH


def exchange_kernel(
    seq_devices, head_devices, chunks,
    q_ref, k_ref, v_ref, pos_ref, rows_ref, cols_ref,
    kbuf, vbuf, pbuf,
    kv_send, kv_recv, line_send, line_recv, tree_send, tree_recv, lane_send, lane_recv,
):
    tokens, width = q_ref.shape
    lanes = head_devices // seq_devices
    bits = seq_devices.bit_length() - 1
    chunk_width = width // chunks
    chunk_heads = chunk_width // HD
    score_scale = HD ** (-0.5)
    head = lax.axis_index("head")
    span = lax.axis_index("seq")
    node, lane = head // lanes, head % lanes
    group = (span // SPANS) * SPANS
    place = span % SPANS

    def flip(bit):
        has = (node // 2**bit) % 2
        return (node + (1 - 2 * has) * 2**bit) * lanes + lane

    far = [(node // 2**bit + span // 2**bit) % 2 for bit in range(bits)]
    above = [sum(far[bit:]) for bit in range(bits)]
    root = above[0] == 0
    not_root = above[0] > 0

    def peer(step):
        return group + (place + step) % SPANS

    def mate(step):
        return node * lanes + (lane + step) % lanes

    barrier = pltpu.get_barrier_semaphore()
    count = 0
    for step in range(1, SPANS):
        pl.semaphore_signal(barrier, inc=1, device_id={"seq": peer(step)}, device_id_type=MESH)
        count += 1
    for bit in range(bits):
        pl.semaphore_signal(barrier, inc=1, device_id={"head": flip(bit)}, device_id_type=MESH)
        count += 1
    for step in range(1, lanes):
        pl.semaphore_signal(barrier, inc=1, device_id={"head": mate(step)}, device_id_type=MESH)
        count += 1
    if seq_devices > SPANS:
        @pl.when(span > 0)
        def _():
            pl.semaphore_signal(barrier, inc=1, device_id={"seq": span - 1}, device_id_type=MESH)

        @pl.when(span < seq_devices - 1)
        def _():
            pl.semaphore_signal(barrier, inc=1, device_id={"seq": span + 1}, device_id_type=MESH)

        @pl.when(span > 0)
        def _():
            pl.semaphore_wait(barrier, 1)

        @pl.when(span < seq_devices - 1)
        def _():
            pl.semaphore_wait(barrier, 1)

    pl.semaphore_wait(barrier, count)
    key_head = head * (width // HD) // (HEADS // KVH)
    key_columns = pl.ds(pl.multiple_of(key_head * HD, HD), HD)

    def kv_copies(step):
        copies = []
        for which, (src, dst) in enumerate((
            (k_ref.at[:, key_columns], kbuf.at[place]),
            (v_ref.at[:, key_columns], vbuf.at[place]),
            (pos_ref, pbuf.at[place]),
        )):
            copies.append(pltpu.make_async_remote_copy(
                src_ref=src, dst_ref=dst,
                send_sem=kv_send.at[which, step - 1], recv_sem=kv_recv.at[which, step - 1],
                device_id={"seq": peer(step)}, device_id_type=MESH,
            ))
        return copies

    def kv_arrivals(step):
        source = (place + SPANS - step) % SPANS
        copies = []
        for which, (src, dst) in enumerate((
            (k_ref.at[:, key_columns], kbuf.at[source]),
            (v_ref.at[:, key_columns], vbuf.at[source]),
            (pos_ref, pbuf.at[source]),
        )):
            copies.append(pltpu.make_async_remote_copy(
                src_ref=src, dst_ref=dst,
                send_sem=kv_send.at[which, step - 1], recv_sem=kv_recv.at[which, step - 1],
                device_id={"seq": peer(step)}, device_id_type=MESH,
            ))
        return copies

    for step in range(1, SPANS):
        for copy in kv_copies(step):
            copy.start()
    kbuf[place] = k_ref[:, key_columns]
    vbuf[place] = v_ref[:, key_columns]
    pbuf[place] = pos_ref[...]

    def row_chunk(block, part):
        return (
            pl.ds(pl.multiple_of(block * tokens, tokens), tokens),
            pl.ds(pl.multiple_of(part * chunk_width, chunk_width), chunk_width),
        )

    def col_chunk(of_lane, block, part):
        return (
            pl.ds(pl.multiple_of(block * tokens, tokens), tokens),
            pl.ds(pl.multiple_of(of_lane * width + part * chunk_width, chunk_width), chunk_width),
        )

    def line_copy(way, block, part):
        where = rows_ref.at[row_chunk(block, part)]
        return pltpu.make_async_remote_copy(
            src_ref=where, dst_ref=where,
            send_sem=line_send.at[way, block, part], recv_sem=line_recv.at[block, part],
            device_id={"seq": span + 1 - 2 * way}, device_id_type=MESH,
        )

    def tree_copy(bit, block, part, source):
        return pltpu.make_async_remote_copy(
            src_ref=source, dst_ref=cols_ref.at[col_chunk(lane, block, part)],
            send_sem=tree_send.at[bit, block, part], recv_sem=tree_recv.at[block, part],
            device_id={"head": flip(bit)}, device_id_type=MESH,
        )

    def lane_copy(step, of_lane, block, part, source):
        return pltpu.make_async_remote_copy(
            src_ref=source, dst_ref=cols_ref.at[col_chunk(of_lane, block, part)],
            send_sem=lane_send.at[step - 1, block, part],
            recv_sem=lane_recv.at[step - 1, block, part],
            device_id={"head": mate(step)}, device_id_type=MESH,
        )

    def spread(block, part, source):
        for bit in range(bits):
            @pl.when(above[bit] == 0)
            def _():
                tree_copy(bit, block, part, source).start()
        for step in range(1, lanes):
            lane_copy(step, lane, block, part, source).start()

    def on_row(block, part, up, down):
        @pl.when(up)
        def _():
            line_copy(0, block, part).start()

        @pl.when(down)
        def _():
            line_copy(1, block, part).start()

        @pl.when(root)
        def _():
            spread(block, part, rows_ref.at[row_chunk(block, part)])
            cols_ref[col_chunk(lane, block, part)] = rows_ref[row_chunk(block, part)]

    has_up = span < seq_devices - 1
    has_down = span > 0

    for step in range(1, SPANS):
        for copy in kv_arrivals(step):
            copy.wait_recv()

    keys = kbuf[...].reshape(SPANS * tokens, HD)
    values = vbuf[...].reshape(SPANS * tokens, HD)
    key_places = jnp.concatenate([pbuf[j] for j in range(SPANS)], axis=1)
    query_places = jnp.broadcast_to(pos_ref[0:1, 0:1], (tokens, 1)) + lax.broadcasted_iota(
        jnp.int32, (tokens, 1), 0
    )
    visible = key_places <= query_places

    def compute(part, carry):
        pieces = []
        for h in range(chunk_heads):
            columns = pl.ds(pl.multiple_of(part * chunk_width + h * HD, HD), HD)
            queries = q_ref[:, columns]
            scores = lax.dot_general(
                queries, keys, (((1,), (1,)), ((), ())), preferred_element_type=jnp.float32
            ) * score_scale
            masked = jnp.where(visible, scores, -jnp.inf)
            row_top = jnp.max(masked, axis=1, keepdims=True)
            weights = jnp.exp(masked - row_top)
            weight_sum = jnp.sum(weights, axis=1, keepdims=True)
            mixed = jnp.dot(
                weights.astype(jnp.bfloat16), values, preferred_element_type=jnp.float32
            )
            pieces.append((mixed / weight_sum).astype(jnp.bfloat16))
        rows_ref[row_chunk(span, part)] = jnp.concatenate(pieces, axis=1)
        on_row(span, part, has_up, has_down)
        return carry

    lax.fori_loop(0, chunks, compute, 0)

    def relay(item, carry):
        back, part = item // chunks, item % chunks
        reach = back + 1

        @pl.when(reach <= span)
        def _():
            block = span - reach
            line_copy(0, block, part).wait_recv()
            on_row(block, part, has_up, False)

        @pl.when(span + reach < seq_devices)
        def _():
            block = span + reach
            line_copy(1, block, part).wait_recv()
            on_row(block, part, False, has_down)

        def from_parent(block):
            source = cols_ref.at[col_chunk(lane, block, part)]
            tree_copy(0, block, part, source).wait_recv()
            spread(block, part, source)

        @pl.when(not_root)
        def _():
            @pl.when(back <= span)
            def _():
                from_parent(span - back)

            @pl.when(jnp.logical_and(back > 0, span + back < seq_devices))
            def _():
                from_parent(span + back)

        return carry

    lax.fori_loop(0, seq_devices * chunks, relay, 0)

    def drain(item, carry):
        block, part = item // chunks, item % chunks
        source = cols_ref.at[col_chunk(lane, block, part)]

        @pl.when(jnp.logical_and(has_up, block <= span))
        def _():
            line_copy(0, block, part).wait_send()

        @pl.when(jnp.logical_and(has_down, block >= span))
        def _():
            line_copy(1, block, part).wait_send()

        for bit in range(bits):
            @pl.when(above[bit] == 0)
            def _():
                tree_copy(bit, block, part, source).wait_send()
        for step in range(1, lanes):
            lane_copy(step, lane, block, part, source).wait_send()
            lane_copy(step, (lane + lanes - step) % lanes, block, part, source).wait_recv()
        return carry

    lax.fori_loop(0, seq_devices * chunks, drain, 0)
    for step in range(1, SPANS):
        for copy in kv_copies(step):
            copy.wait_send()


def on_device(query_rows, key_rows, value_rows, positions):
    tokens, width = query_rows.shape
    seq_devices = lax.axis_size("seq")
    head_devices = lax.axis_size("head")
    lanes = head_devices // seq_devices
    bits = seq_devices.bit_length() - 1
    chunks = max(1, width // (4 * HD))
    vmem = pl.BlockSpec(memory_space=pltpu.VMEM)
    dma = pltpu.SemaphoreType.DMA
    rows, cols = pl.pallas_call(
        functools.partial(exchange_kernel, seq_devices, head_devices, chunks),
        out_shape=(
            jax.ShapeDtypeStruct((seq_devices * tokens, width), jnp.bfloat16),
            jax.ShapeDtypeStruct((seq_devices * tokens, lanes * width), jnp.bfloat16),
        ),
        in_specs=[vmem] * 4,
        out_specs=(vmem, vmem),
        scratch_shapes=[
            pltpu.VMEM((SPANS, tokens, HD), jnp.bfloat16),
            pltpu.VMEM((SPANS, tokens, HD), jnp.bfloat16),
            pltpu.VMEM((SPANS, 1, tokens), jnp.int32),
            dma((3, SPANS - 1)),
            dma((3, SPANS - 1)),
            dma((2, seq_devices, chunks)),
            dma((seq_devices, chunks)),
            dma((bits, seq_devices, chunks)),
            dma((seq_devices, chunks)),
            dma((lanes - 1, seq_devices, chunks)),
            dma((lanes - 1, seq_devices, chunks)),
        ],
        compiler_params=pltpu.CompilerParams(collective_id=0, has_side_effects=True),
        name="attend_exchange",
    )(query_rows, key_rows, value_rows, positions.reshape(1, tokens))
    attended = lax.dynamic_slice_in_dim(rows, lax.axis_index("seq") * tokens, tokens, 0)
    hessian = lax.dot_general(
        rows, cols, (((0,), (0,)), ((), ())), preferred_element_type=jnp.float32
    )
    return (attended, hessian)


def solution(mesh):
    placed = (P("seq", "head"), P("seq", None), P("seq", None), P("seq"))
    return jax.shard_map(
        on_device,
        mesh=mesh,
        in_specs=placed,
        out_specs=(P("seq", "head"), P("head", "seq")),
        check_vma=False,
    )
```

```python
import functools

import jax
import jax.numpy as jnp
from jax import lax
from jax.experimental import pallas as pl
from jax.experimental.pallas import tpu as pltpu
from jax.sharding import PartitionSpec as P

HEADS = 128
KVH = 8
HD = 128
SPANS = 4
CHUNK_HEADS = 4
TILE = 512
MESH = pl.DeviceIdType.MESH


def exchange_kernel(
    seq_devices, head_devices, chunks,
    q_ref, k_ref, v_ref, pos_ref, attended_ref, turned_ref, cols_ref,
    rows_ref, kbuf, vbuf, pbuf,
    kv_send, kv_recv, line_send, line_recv, tree_send, tree_recv, lane_send, lane_recv,
):
    tokens, width = q_ref.shape
    lanes = head_devices // seq_devices
    bits = seq_devices.bit_length() - 1
    chunk_width = width // chunks
    chunk_heads = chunk_width // HD
    score_scale = HD ** (-0.5)
    head = lax.axis_index("head")
    span = lax.axis_index("seq")
    node, lane = head // lanes, head % lanes
    group = (span // SPANS) * SPANS
    place = span % SPANS

    def flip(bit):
        has = (node // 2**bit) % 2
        return (node + (1 - 2 * has) * 2**bit) * lanes + lane

    far = [(node // 2**bit + span // 2**bit) % 2 for bit in range(bits)]
    above = [sum(far[bit:]) for bit in range(bits)]
    below = [sum(far[: bit + 1]) for bit in range(bits)]
    root = above[0] == 0
    not_root = above[0] > 0

    def peer(step):
        return group + (place + step) % SPANS

    def mate(step):
        return node * lanes + (lane + step) % lanes

    barrier = pltpu.get_barrier_semaphore()
    count = 0
    for step in range(1, SPANS):
        pl.semaphore_signal(barrier, inc=1, device_id={"seq": peer(step)}, device_id_type=MESH)
        count += 1
    for bit in range(bits):
        pl.semaphore_signal(barrier, inc=1, device_id={"head": flip(bit)}, device_id_type=MESH)
        count += 1
    for step in range(1, lanes):
        pl.semaphore_signal(barrier, inc=1, device_id={"head": mate(step)}, device_id_type=MESH)
        count += 1
    if seq_devices > SPANS:
        @pl.when(span > 0)
        def _():
            pl.semaphore_signal(barrier, inc=1, device_id={"seq": span - 1}, device_id_type=MESH)

        @pl.when(span < seq_devices - 1)
        def _():
            pl.semaphore_signal(barrier, inc=1, device_id={"seq": span + 1}, device_id_type=MESH)

        @pl.when(span > 0)
        def _():
            pl.semaphore_wait(barrier, 1)

        @pl.when(span < seq_devices - 1)
        def _():
            pl.semaphore_wait(barrier, 1)

    pl.semaphore_wait(barrier, count)
    key_head = head * (width // HD) // (HEADS // KVH)
    key_columns = pl.ds(pl.multiple_of(key_head * HD, HD), HD)

    def kv_copies(step):
        copies = []
        for which, (src, dst) in enumerate((
            (k_ref.at[:, key_columns], kbuf.at[place]),
            (v_ref.at[:, key_columns], vbuf.at[place]),
            (pos_ref, pbuf.at[place]),
        )):
            copies.append(pltpu.make_async_remote_copy(
                src_ref=src, dst_ref=dst,
                send_sem=kv_send.at[which, step - 1], recv_sem=kv_recv.at[which, step - 1],
                device_id={"seq": peer(step)}, device_id_type=MESH,
            ))
        return copies

    def kv_arrivals(step):
        source = (place + SPANS - step) % SPANS
        copies = []
        for which, (src, dst) in enumerate((
            (k_ref.at[:, key_columns], kbuf.at[source]),
            (v_ref.at[:, key_columns], vbuf.at[source]),
            (pos_ref, pbuf.at[source]),
        )):
            copies.append(pltpu.make_async_remote_copy(
                src_ref=src, dst_ref=dst,
                send_sem=kv_send.at[which, step - 1], recv_sem=kv_recv.at[which, step - 1],
                device_id={"seq": peer(step)}, device_id_type=MESH,
            ))
        return copies

    for step in range(1, SPANS):
        for copy in kv_copies(step):
            copy.start()
    kbuf[place] = k_ref[:, key_columns]
    vbuf[place] = v_ref[:, key_columns]
    pbuf[place] = pos_ref[...]

    def row_chunk(block, part):
        return (
            pl.ds(pl.multiple_of(block * tokens, tokens), tokens),
            pl.ds(pl.multiple_of(part * chunk_width, chunk_width), chunk_width),
        )

    def col_chunk(of_lane, block, part):
        return (
            pl.ds(pl.multiple_of(block * tokens, tokens), tokens),
            pl.ds(pl.multiple_of(of_lane * width + part * chunk_width, chunk_width), chunk_width),
        )

    def line_copy(way, block, part):
        where = rows_ref.at[row_chunk(block, part)]
        return pltpu.make_async_remote_copy(
            src_ref=where, dst_ref=where,
            send_sem=line_send.at[way, block, part], recv_sem=line_recv.at[block, part],
            device_id={"seq": span + 1 - 2 * way}, device_id_type=MESH,
        )

    def tree_copy(bit, block, part, source):
        return pltpu.make_async_remote_copy(
            src_ref=source, dst_ref=cols_ref.at[col_chunk(lane, block, part)],
            send_sem=tree_send.at[bit, block, part], recv_sem=tree_recv.at[block, part],
            device_id={"head": flip(bit)}, device_id_type=MESH,
        )

    def lane_copy(step, of_lane, block, part, source):
        return pltpu.make_async_remote_copy(
            src_ref=source, dst_ref=cols_ref.at[col_chunk(of_lane, block, part)],
            send_sem=lane_send.at[step - 1, block, part],
            recv_sem=lane_recv.at[step - 1, block, part],
            device_id={"head": mate(step)}, device_id_type=MESH,
        )

    def sends(bit, block, part):
        turn = (block + part) % 2
        return turn * above[bit] + (1 - turn) * below[bit] == 0

    def spread(block, part, source):
        for bit in range(bits):
            @pl.when(sends(bit, block, part))
            def _():
                tree_copy(bit, block, part, source).start()
        for step in range(1, lanes):
            lane_copy(step, lane, block, part, source).start()

    def on_row(block, part, up, down):
        @pl.when(up)
        def _():
            line_copy(0, block, part).start()

        @pl.when(down)
        def _():
            line_copy(1, block, part).start()

        @pl.when(root)
        def _():
            spread(block, part, rows_ref.at[row_chunk(block, part)])
            cols_ref[col_chunk(lane, block, part)] = rows_ref[row_chunk(block, part)]

        turned_ref[
            pl.ds(pl.multiple_of(part * chunk_width, chunk_width), chunk_width),
            pl.ds(pl.multiple_of(block * tokens, tokens), tokens),
        ] = rows_ref[row_chunk(block, part)].T

    has_up = span < seq_devices - 1
    has_down = span > 0

    for step in range(1, SPANS):
        for copy in kv_arrivals(step):
            copy.wait_recv()

    keys = kbuf[...].reshape(SPANS * tokens, HD)
    values = vbuf[...].reshape(SPANS * tokens, HD)
    key_places = jnp.concatenate([pbuf[j] for j in range(SPANS)], axis=1)
    query_places = jnp.broadcast_to(pos_ref[0:1, 0:1], (tokens, 1)) + lax.broadcasted_iota(
        jnp.int32, (tokens, 1), 0
    )
    visible = key_places <= query_places

    def compute(part, carry):
        pieces = []
        for h in range(chunk_heads):
            columns = pl.ds(pl.multiple_of(part * chunk_width + h * HD, HD), HD)
            queries = q_ref[:, columns]
            scores = lax.dot_general(
                queries, keys, (((1,), (1,)), ((), ())), preferred_element_type=jnp.float32
            ) * score_scale
            masked = jnp.where(visible, scores, -jnp.inf)
            row_top = jnp.max(masked, axis=1, keepdims=True)
            weights = jnp.exp(masked - row_top)
            weight_sum = jnp.sum(weights, axis=1, keepdims=True)
            mixed = jnp.dot(
                weights.astype(jnp.bfloat16), values, preferred_element_type=jnp.float32
            )
            pieces.append((mixed / weight_sum).astype(jnp.bfloat16))
        joined = jnp.concatenate(pieces, axis=1)
        rows_ref[row_chunk(span, part)] = joined
        attended_ref[:, pl.ds(pl.multiple_of(part * chunk_width, chunk_width), chunk_width)] = joined

        on_row(span, part, has_up, has_down)
        return carry

    lax.fori_loop(0, chunks, compute, 0)

    def relay(item, carry):
        back, part = item // chunks, item % chunks
        reach = back + 1

        @pl.when(reach <= span)
        def _():
            block = span - reach
            line_copy(0, block, part).wait_recv()
            on_row(block, part, has_up, False)

        @pl.when(span + reach < seq_devices)
        def _():
            block = span + reach
            line_copy(1, block, part).wait_recv()
            on_row(block, part, False, has_down)

        @pl.when(jnp.logical_and(not_root, item >= chunks))
        def _():
            late = back - 1

            def from_parent(block):
                source = cols_ref.at[col_chunk(lane, block, part)]
                tree_copy(0, block, part, source).wait_recv()
                spread(block, part, source)

            @pl.when(late <= span)
            def _():
                from_parent(span - late)

            @pl.when(jnp.logical_and(late > 0, span + late < seq_devices))
            def _():
                from_parent(span + late)

        return carry

    lax.fori_loop(0, (seq_devices + 1) * chunks, relay, 0)

    def drain(item, carry):
        block, part = item // chunks, item % chunks
        source = cols_ref.at[col_chunk(lane, block, part)]

        @pl.when(jnp.logical_and(has_up, block <= span))
        def _():
            line_copy(0, block, part).wait_send()

        @pl.when(jnp.logical_and(has_down, block >= span))
        def _():
            line_copy(1, block, part).wait_send()

        for bit in range(bits):
            @pl.when(sends(bit, block, part))
            def _():
                tree_copy(bit, block, part, source).wait_send()
        for step in range(1, lanes):
            lane_copy(step, lane, block, part, source).wait_send()
            lane_copy(step, (lane + lanes - step) % lanes, block, part, source).wait_recv()
        return carry

    lax.fori_loop(0, seq_devices * chunks, drain, 0)

    for step in range(1, SPANS):
        for copy in kv_copies(step):
            copy.wait_send()


def hessian_kernel(own_ref, turned_ref, cols_ref, attended_ref, out_ref):
    @pl.when(pl.program_id(0) == 0)
    def _():
        attended_ref[...] = own_ref[...]

    out_ref[...] = jnp.dot(turned_ref[...], cols_ref[...], preferred_element_type=jnp.float32)


def on_device(query_rows, key_rows, value_rows, positions):
    tokens, width = query_rows.shape
    seq_devices = lax.axis_size("seq")
    head_devices = lax.axis_size("head")
    lanes = head_devices // seq_devices
    bits = seq_devices.bit_length() - 1
    chunks = max(1, width // (CHUNK_HEADS * HD))
    vmem = pl.BlockSpec(memory_space=pltpu.VMEM)
    dma = pltpu.SemaphoreType.DMA
    own, turned, cols = pl.pallas_call(
        functools.partial(exchange_kernel, seq_devices, head_devices, chunks),
        out_shape=(
            jax.ShapeDtypeStruct((tokens, width), jnp.bfloat16),
            jax.ShapeDtypeStruct((width, seq_devices * tokens), jnp.bfloat16),
            jax.ShapeDtypeStruct((seq_devices * tokens, lanes * width), jnp.bfloat16),
        ),
        in_specs=[vmem] * 4,
        out_specs=(vmem, vmem, vmem),
        scratch_shapes=[
            pltpu.VMEM((seq_devices * tokens, width), jnp.bfloat16),
            pltpu.VMEM((SPANS, tokens, HD), jnp.bfloat16),
            pltpu.VMEM((SPANS, tokens, HD), jnp.bfloat16),
            pltpu.VMEM((SPANS, 1, tokens), jnp.int32),
            dma((3, SPANS - 1)),
            dma((3, SPANS - 1)),
            dma((2, seq_devices, chunks)),
            dma((seq_devices, chunks)),
            dma((bits, seq_devices, chunks)),
            dma((seq_devices, chunks)),
            dma((lanes - 1, seq_devices, chunks)),
            dma((lanes - 1, seq_devices, chunks)),
        ],
        compiler_params=pltpu.CompilerParams(collective_id=0, has_side_effects=True),
        name="attend_exchange",
    )(query_rows, key_rows, value_rows, positions.reshape(1, tokens))
    depth, breadth = cols.shape
    tile = min(TILE, breadth)
    attended, hessian = pl.pallas_call(
        hessian_kernel,
        grid=(breadth // tile,),
        out_shape=(
            jax.ShapeDtypeStruct((tokens, width), jnp.bfloat16),
            jax.ShapeDtypeStruct((width, breadth), jnp.float32),
        ),
        in_specs=[
            pl.BlockSpec((tokens, width), lambda j: (0, 0)),
            pl.BlockSpec((width, depth), lambda j: (0, 0)),
            pl.BlockSpec((depth, tile), lambda j: (0, j)),
        ],
        out_specs=(
            pl.BlockSpec((tokens, width), lambda j: (0, 0)),
            pl.BlockSpec((width, tile), lambda j: (0, j)),
        ),
        name="hessian",
    )(own, turned, cols)
    return (attended, hessian)


def solution(mesh):
    placed = (P("seq", "head"), P("seq", None), P("seq", None), P("seq"))
    return jax.shard_map(
        on_device,
        mesh=mesh,
        in_specs=placed,
        out_specs=(P("seq", "head"), P("head", "seq")),
        check_vma=False,
    )
```
